32 devices in a mesh: rep: 2 (over z, core), dp: 16 (over x, y).
Axes of the slice: x: 4, y: 4, z: 1, core: 2. Of those that a mesh axis runs over, the one named last changes fastest.
The devices are a block of a 4x4x8 slice.
Arguments:
- x: bfloat16 [32, 4096, 896], P(('rep', 'dp')), parts along dimension 0
- dy: bfloat16 [32, 4096, 896], P(('rep', 'dp')), parts along dimension 0
- w_gate: bfloat16 [2, 896, 2304], P(None, 'dp')
- w_up: bfloat16 [2, 896, 2304], P(None, 'dp')
- w_down: bfloat16 [2, 2304, 896], P(None, 'dp')
Outputs:
- output 1: bfloat16 [32, 4096, 896], P(('rep', 'dp')), parts along dimension 0
- output 2: bfloat16 [4, 896, 2304], P('rep', 'dp'), parts along dimension 0
- output 3: bfloat16 [4, 896, 2304], P('rep', 'dp'), parts along dimension 0
- output 4: bfloat16 [4, 2304, 896], P('rep', 'dp'), parts along dimension 0
There are 2 independent parts. The reference program is written for one: setup_inputs(seed, part) draws one part's arguments, and reference() takes and returns one part's arrays. A program takes and returns all parts, laid end to end along the dimension named above; an argument that names none is the same for every part.
All inputs are finite; a program needn't handle non-finite values.
Results may differ from the reference program's by a relative error of at most 0.018.
Values are sent between devices in bfloat16 or wider.
A program may use at most 768 MiB of HBM per device.

```python
import jax
import jax.numpy as jnp
from jax import lax

SEQUENCES = 16
TOKENS = 4096
D = 896
FF = 2304
LAYERS = 2
NAMES = ("w_gate", "w_up", "w_down")
SHAPES = {"w_gate": (LAYERS, D, FF), "w_up": (LAYERS, D, FF), "w_down": (LAYERS, FF, D)}


def bump(key, n, height):
    away = (jnp.arange(n, dtype=jnp.int32) - jax.random.randint(key, (), 0, n, jnp.int32)) % n
    return jnp.where(away < n // 8, height, 1.0)


def together(key, own, strength):
    shared = jax.random.normal(key, own.shape[1:], jnp.float32)
    return (own + strength * shared) * lax.rsqrt(1 + strength * strength)


def setup_inputs(seed: int = 0, part: int = 0) -> dict:
    kx, kdy, ka, kb, kz, kf, kh, kl, *kw = jax.random.split(jax.random.key(seed), 8 + len(NAMES))
    kx, kdy, ka, kb = (jax.random.fold_in(k, part) for k in (kx, kdy, ka, kb))
    shape = (SEQUENCES, TOKENS, D)
    much_x, much_dy = jax.random.uniform(kz, (2,), jnp.float32, 0.0, 1.0)
    layers = 2.0 ** jax.random.uniform(kl, (LAYERS, 1, 1), jnp.float32, -1.0, 1.0)
    x = together(ka, jax.random.normal(kx, shape, jnp.float32), much_x) * bump(kf, D, 4.0)
    dy = together(kb, jax.random.normal(kdy, shape, jnp.float32), much_dy)
    drawn = {"x": x.astype(jnp.bfloat16), "dy": (dy * (SEQUENCES * TOKENS) ** -0.5).astype(jnp.bfloat16)}
    for key, name in zip(kw, NAMES, strict=True):
        w = jax.random.normal(key, SHAPES[name], jnp.float32) * SHAPES[name][1] ** -0.5
        drawn[name] = (w * {"w_gate": 1.0, "w_up": bump(kh, FF, 4.0), "w_down": layers}[name]).astype(jnp.bfloat16)
    return drawn


def matmul(a, w):
    return jnp.dot(a, w, preferred_element_type=jnp.float32).astype(jnp.bfloat16)


def normed(h):
    wide = h.astype(jnp.float32)
    scale = lax.rsqrt(jnp.mean(wide**2, -1, keepdims=True) + 1e-6)
    return (wide * scale).astype(jnp.bfloat16)


def layer(h, w):
    a = normed(h)
    gate = jnp.dot(a, w["w_gate"], preferred_element_type=jnp.float32)
    up = jnp.dot(a, w["w_up"], preferred_element_type=jnp.float32)
    return h + matmul((jax.nn.silu(gate) * up).astype(jnp.bfloat16), w["w_down"])


def stack(weights, h):
    return lax.scan(lambda h, w: (layer(h, w), None), h, weights)[0]


def reference(x, dy, w_gate, w_up, w_down):
    weights = dict(zip(NAMES, (w_gate, w_up, w_down), strict=True))

    def take(so_far, sequence):
        h, by_y = sequence
        _, back = jax.vjp(stack, weights, h)
        by_weights, by_h = back(by_y)
        return jax.tree.map(lambda total, term: total + term.astype(jnp.float32), so_far, by_weights), by_h

    none_yet = {name: jnp.zeros(w.shape, jnp.float32) for name, w in weights.items()}
    by_weights, by_x = lax.scan(take, none_yet, (x, dy))
    return (by_x, *(by_weights[name].astype(jnp.bfloat16) for name in NAMES))
```

```python
import functools
import math

import jax
import jax.numpy as jnp
from jax import lax
from jax.experimental import pallas as pl
from jax.experimental.pallas import tpu as pltpu
from jax.sharding import PartitionSpec as P

F32, BF16 = jnp.float32, jnp.bfloat16
ANY = pl.ANY
LIMIT = 64 * 1024 * 1024
NT = (((1,), (1,)), ((), ()))


def dot(a, b):
    return jnp.dot(a, b, preferred_element_type=F32)


def dot_nt(a, b):
    return lax.dot_general(a, b, NT, preferred_element_type=F32)


class Gather:
    def __init__(self, n, layer, shards, outs, sems):
        self.n, self.layer, self.shards, self.outs = n, layer, shards, outs
        self.send, self.recv, self.local = sems
        side = math.isqrt(n)
        self.side = side
        rep, dp = lax.axis_index("rep"), lax.axis_index("dp")
        self.core = lax.rem(rep, 2)
        self.rep, self.partner = rep, rep + 1 - 2 * self.core
        self.i, self.j = dp // side, lax.rem(dp, side)
        self.dp = dp

    @staticmethod
    def sems(n, matrices):
        side = math.isqrt(n)
        k = matrices * (4 + 4 * side + n - 1)
        return [pltpu.SemaphoreType.DMA((k,)), pltpu.SemaphoreType.DMA((k,)), pltpu.SemaphoreType.DMA((matrices,))]

    def at(self, a, b):
        s, c = self.side, self.core
        i = lax.rem(self.i + c * a + (1 - c) * b + 2 * s, s)
        j = lax.rem(self.j + (1 - c) * a + c * b + 2 * s, s)
        return i * s + j

    def piece(self, m, block, core, part=None, shard=False):
        rows = self.shards[m].shape[1]
        cols = self.shards[m].shape[2]
        if cols % 256 == 0:
            col, wide = pl.multiple_of(core * (cols // 2), 128), cols // 2
            first, high = 0, rows
        else:
            col, wide = 0, cols
            first, high = core * (rows // 2), rows // 2
        cut = (high // 2 + 7) // 8 * 8
        if part is not None:
            first, high = (first, cut) if part == 0 else (first + cut, high - cut)
        if shard:
            return self.shards[m].at[self.layer, pl.ds(pl.multiple_of(first, 8), high), pl.ds(col, wide)]
        return self.outs[m].at[pl.ds(pl.multiple_of(block * rows + first, 8), high), pl.ds(col, wide)]

    def copy(self, slot, src, dst, dp, rep=None):
        rep = self.rep if rep is None else rep
        return pltpu.make_async_remote_copy(
            src_ref=src, dst_ref=dst, send_sem=self.send.at[slot], recv_sem=self.recv.at[slot],
            device_id=(rep, dp), device_id_type=pl.DeviceIdType.MESH)

    def each(self, kind, a=0, b=0):
        s = self.side
        out = []
        for m in range(len(self.shards)):
            base = m * (4 + 4 * s + self.n - 1)
            for k, d in enumerate((1, -1)):
                if kind == "first":
                    out.append((base + k, self.piece(m, self.dp, self.core, shard=True), self.piece(m, self.dp, self.core),
                                self.at(d, 0), self.piece(m, self.at(-d, 0), self.core)))
                if kind == "first_on":
                    block = self.piece(m, self.at(-d, 0), self.core, k)
                    out.append((base + 2 + k, block, block, self.at(d, 0), self.piece(m, self.at(2, 0), self.core, k)))
                if kind == "second":
                    block = self.piece(m, self.at(a, 0), self.core)
                    src = self.piece(m, self.dp, self.core, shard=True) if a == 0 else block
                    out.append((base + 4 + 2 * a + k, src, block, self.at(0, d), self.piece(m, self.at(a, -d), self.core)))
                if kind == "second_on":
                    block = self.piece(m, self.at(a, -d), self.core, k)
                    out.append((base + 4 + 2 * s + 2 * a + k, block, block, self.at(0, d), self.piece(m, self.at(a, 2), self.core, k)))
            if kind == "pair":
                block = self.piece(m, self.at(a, b), self.core)
                out.append((base + 4 + 4 * s + a * s + b - 1, block, block, None, self.piece(m, self.at(b, a), 1 - self.core)))
        return out

    def target(self, dp):
        return (dp, None) if dp is not None else (self.dp, self.partner)

    def start(self, *kinds):
        for kind in kinds:
            for slot, src, dst, dp, _ in self.each(*kind):
                self.copy(slot, src, dst, *self.target(dp)).start()

    def arrived(self, *kinds):
        for kind in kinds:
            for slot, _, _, dp, here in self.each(*kind):
                self.copy(slot, here, here, *self.target(dp)).wait_recv()

    def sent(self, *kinds):
        for kind in kinds:
            for slot, src, dst, dp, _ in self.each(*kind):
                self.copy(slot, src, dst, *self.target(dp)).wait_send()

    def own(self):
        out = []
        for m in range(len(self.shards)):
            rows = self.shards[m].shape[1]
            out.append(pltpu.make_async_copy(self.shards[m].at[self.layer],
                                             self.outs[m].at[pl.ds(pl.multiple_of(self.dp * rows, 8), rows)], self.local.at[m]))
        return out

    def stages(self):
        s = self.side
        pairs = [("pair", a, b) for a in range(s) for b in range(s) if a or b]
        ahead = [("first",), ("first_on",)] + [(kind, a) for kind in ("second", "second_on") for a in range(s)]

        def begin():
            barrier = pltpu.get_barrier_semaphore()
            for a, b in ((1, 0), (-1, 0), (0, 1), (0, -1)):
                pl.semaphore_signal(barrier, inc=1, device_id=(self.rep, self.at(a, b)), device_id_type=pl.DeviceIdType.MESH)
            pl.semaphore_signal(barrier, inc=1, device_id=(self.partner, self.dp), device_id_type=pl.DeviceIdType.MESH)
            pl.semaphore_wait(barrier, 5)
            self.start(("first",), ("second", 0))
            for c in self.own():
                c.start()

        def end():
            self.arrived(*pairs)
            self.sent(*ahead, *pairs)
            for c in self.own():
                c.wait()

        def stage(here, on):
            def run():
                self.arrived(*here)
                self.start(*on)
            return run

        near = (1, s - 1)
        return [
            begin,
            stage([("first",)], [("first_on",)] + [("second", a) for a in near] + [("pair", a, 0) for a in near]),
            stage([("second", 0)], [("second_on", 0)] + [("pair", 0, b) for b in near]),
            stage([("first_on",)], [("second", 2), ("pair", 2, 0)]),
            stage([("second", a) for a in near], [("second_on", a) for a in near] + [("pair", a, b) for a in near for b in near]),
            stage([("second_on", 0)], [("pair", 0, 2)]),
            stage([("second", 2)], [("second_on", 2)] + [("pair", 2, b) for b in near]),
            stage([("second_on", a) for a in near], [("pair", a, 2) for a in near]),
            stage([("second_on", 2)], [("pair", 2, 2)]),
            end]


def gathered(shards, n):
    return [jax.ShapeDtypeStruct((w.shape[1] * n, w.shape[2]), w.dtype) for w in shards]


def gather(n, layer, shards):
    M = len(shards)

    def kernel(*refs):
        for stage in Gather(n, layer, refs[:M], refs[M:2 * M], refs[2 * M:]).stages():
            stage()

    return pl.pallas_call(
        kernel, out_shape=gathered(shards, n), in_specs=[pl.BlockSpec(memory_space=ANY)] * M,
        out_specs=[pl.BlockSpec(memory_space=ANY)] * M, scratch_shapes=Gather.sems(n, M), name="gather",
        compiler_params=pltpu.CompilerParams(collective_id=1, has_side_effects=True))(*shards)


class Reduce:
    def __init__(self, n, terms, outs, buffers, sems, greet=True):
        self.n, self.terms, self.outs, self.buffers, self.greet = n, terms, outs, buffers, greet
        self.send, self.recv, self.local = sems
        self.place = Gather.__new__(Gather)
        side = math.isqrt(n)
        rep, dp = lax.axis_index("rep"), lax.axis_index("dp")
        p = self.place
        p.side, p.core, p.rep, p.dp, p.i, p.j = side, lax.rem(rep, 2), rep, dp, dp // side, lax.rem(dp, side)
        self.at, self.rep, self.side = p.at, rep, side

    @staticmethod
    def part_shape(shape, n):
        rows, cols = shape[0] // n, shape[1]
        return (rows, cols // 2) if cols % 256 == 0 else (rows // 2, cols)

    @staticmethod
    def scratch(shapes, n):
        side = math.isqrt(n)
        out = []
        for shape in shapes:
            p = Reduce.part_shape(shape, n)
            out += [pltpu.VMEM(lead + p, BF16) for lead in
                    ((2, side), (2, side), (2, 2, side), (2, side), (2,), (2,), (2, 2), (2, 2))]
        k = len(shapes)
        return out + [pltpu.SemaphoreType.DMA((k * (6 * side + 4),)), pltpu.SemaphoreType.DMA((k * (6 * side + 4),)),
                      pltpu.SemaphoreType.DMA((k * 4 * side,))]

    def term(self, m, block, part):
        rows, cols = self.terms[m].shape[0] // self.n, self.terms[m].shape[1]
        first = block * rows
        high, wide = self.part_shape(self.terms[m].shape, self.n)
        if wide == cols:
            return self.terms[m].at[pl.ds(pl.multiple_of(first + part * high, 8), high)]
        return self.terms[m].at[pl.ds(pl.multiple_of(first, 8), high), pl.ds(part * wide, wide)]

    def copies(self, what):
        s = self.side
        out = []
        for m in range(len(self.terms)):
            r1, own1, r2, own2, s3, r3, s4, r4 = self.buffers[8 * m:8 * m + 8]
            base = m * (6 * s + 4)
            for k, d in enumerate((1, -1)):
                first, second = self.at(d, 0), self.at(0, d)
                for b in range(s):
                    if what == "far":
                        out.append((base + k * s + b, self.term(m, self.at(2, b), k), r1.at[k, b], first))
                    if what == "raw":
                        out.append((base + 2 * s + k * s + b, self.term(m, self.at(d, b), 1 - k), r2.at[k, 1 - k, b], first))
                    if what == "near":
                        out.append((base + 4 * s + k * s + b, r1.at[k, b], r2.at[k, k, b], first))
                if what == "far2":
                    out.append((base + 6 * s + k, s3.at[k], r3.at[k], second))
                if what == "near2":
                    out.append((base + 6 * s + 2 + k, s4.at[k], r4.at[k], second))
        return [pltpu.make_async_remote_copy(src_ref=src, dst_ref=dst, send_sem=self.send.at[i], recv_sem=self.recv.at[i],
                                             device_id=(self.rep, dp), device_id_type=pl.DeviceIdType.MESH)
                for i, src, dst, dp in out]

    def own(self):
        s = self.side
        out = []
        for m in range(len(self.terms)):
            _, own1, _, own2 = self.buffers[8 * m:8 * m + 4]
            for k, d in enumerate((1, -1)):
                for b in range(s):
                    out.append((self.term(m, self.at(d, b), k), own1.at[k, b]))
                    out.append((self.term(m, self.at(0, b), k), own2.at[k, b]))
        return [pltpu.make_async_copy(src, dst, self.local.at[i]) for i, (src, dst) in enumerate(out)]

    def stages(self):
        s, M = self.side, len(self.terms)

        def total(m, part, b):
            _, _, r2, own2 = self.buffers[8 * m:8 * m + 4]
            return own2[part, b].astype(F32) + r2[0, part, b].astype(F32) + r2[1, part, b].astype(F32)

        def begin():
            if self.greet:
                barrier = pltpu.get_barrier_semaphore()
                for a, b in ((1, 0), (-1, 0), (0, 1), (0, -1)):
                    pl.semaphore_signal(barrier, inc=1, device_id=(self.rep, self.at(a, b)), device_id_type=pl.DeviceIdType.MESH)
                pl.semaphore_wait(barrier, 4)
            for c in self.copies("far") + self.copies("raw") + self.own():
                c.start()

        def one():
            for c in self.own():
                c.wait()
            for c in self.copies("far"):
                c.wait_recv()
            for m in range(M):
                r1, own1 = self.buffers[8 * m:8 * m + 2]
                for k in range(2):
                    for b in range(s):
                        r1[k, b] = (r1[k, b].astype(F32) + own1[k, b].astype(F32)).astype(BF16)
            for c in self.copies("near"):
                c.start()

        def two():
            for c in self.copies("raw") + self.copies("near"):
                c.wait_recv()
            for m in range(M):
                s3 = self.buffers[8 * m + 4]
                for k in range(2):
                    s3[k] = total(m, k, 2).astype(BF16)
            for c in self.copies("far2"):
                c.start()

        def three():
            for c in self.copies("far2"):
                c.wait_recv()
            for m in range(M):
                r3, s4 = self.buffers[8 * m + 5:8 * m + 7]
                for k, b in enumerate((1, s - 1)):
                    s4[k, k] = (total(m, k, b) + r3[k].astype(F32)).astype(BF16)
                    s4[k, 1 - k] = total(m, 1 - k, b).astype(BF16)
            for c in self.copies("near2"):
                c.start()

        def four():
            for c in self.copies("near2"):
                c.wait_recv()
            for m in range(M):
                r4 = self.buffers[8 * m + 7]
                high, wide = self.part_shape(self.terms[m].shape, self.n)
                for part in range(2):
                    block = (total(m, part, 0) + r4[0, part].astype(F32) + r4[1, part].astype(F32)).astype(BF16)
                    if wide == self.terms[m].shape[1]:
                        self.outs[m][part * high:(part + 1) * high, :] = block
                    else:
                        self.outs[m][:, part * wide:(part + 1) * wide] = block
            for kind in ("far", "raw", "near", "far2", "near2"):
                for c in self.copies(kind):
                    c.wait_send()

        return [begin, one, two, three, four]


def reduced(terms, n):
    return [jax.ShapeDtypeStruct((t.shape[0] // n, t.shape[1]), BF16) for t in terms]


def spread(stages, when):
    for at, stage in zip(when, stages):
        pl.when(pl.program_id(0) == at)(stage)


def scaled(h):
    wide = h.astype(F32)
    scale = lax.rsqrt(jnp.mean(wide * wide, -1, keepdims=True) + 1e-6)
    return wide, scale, (wide * scale).astype(BF16)


def whole(shape):
    return pl.BlockSpec(shape, lambda i: (0,) * len(shape), pipeline_mode=pl.Buffered(1))


def forward(n, x, wg, wu, wd, shards, tile, step):
    tokens, d = x.shape
    ff = wg.shape[1]
    M = len(shards)
    tiles = tokens // tile
    when = [round(f * (tiles - 1) / 7) for f in (0, 1, 1, 2, 3, 3, 4, 4, 5, 7)]

    def kernel(x_ref, wg_ref, wu_ref, wd_ref, *refs):
        y_ref, gate_ref, up_ref = refs[M:M + 3]
        g = Gather(n, 1, refs[:M], refs[M + 3:2 * M + 3], refs[2 * M + 3:])
        stages = g.stages()
        for at, stage in list(zip(when, stages))[:-1]:
            pl.when(pl.program_id(0) == at)(stage)
        h = x_ref[...]
        _, _, a = scaled(h)
        total = jnp.zeros((tile, d), F32)
        for c in range(0, ff, step):
            gate, up = dot(a, wg_ref[:, c:c + step]), dot(a, wu_ref[:, c:c + step])
            gate_ref[:, c:c + step], up_ref[:, c:c + step] = gate, up
            p = (gate * jax.nn.sigmoid(gate) * up).astype(BF16)
            total += dot(p, wd_ref[c:c + step, :])
        y_ref[...] = h + total.astype(BF16)
        pl.when(pl.program_id(0) == when[-1])(stages[-1])

    rows, broad = pl.BlockSpec((tile, d), lambda i: (i, 0)), pl.BlockSpec((tile, ff), lambda i: (i, 0))
    return pl.pallas_call(
        kernel, grid=(tiles,),
        out_shape=[jax.ShapeDtypeStruct(x.shape, BF16)] + [jax.ShapeDtypeStruct((tokens, ff), F32)] * 2 + gathered(shards, n),
        in_specs=[rows, whole(wg.shape), whole(wu.shape), whole(wd.shape)] + [pl.BlockSpec(memory_space=ANY)] * M,
        out_specs=[rows, broad, broad] + [pl.BlockSpec(memory_space=ANY)] * M, scratch_shapes=Gather.sems(n, M), name="forward",
        cost_estimate=pl.CostEstimate(flops=6 * tokens * d * ff, bytes_accessed=4 * tokens * d + 6 * d * ff, transcendentals=0),
        compiler_params=pltpu.CompilerParams(collective_id=2, has_side_effects=True, vmem_limit_bytes=LIMIT))(x, wg, wu, wd, *shards)


def hidden(gate, up, do, wd, part):
    dp = dot_nt(do, wd[part, :]).astype(BF16).astype(F32)
    sig = jax.nn.sigmoid(gate)
    silu = gate * sig
    return (silu * up).astype(BF16), (dp * up * (sig * (1 + gate * (1 - sig)))).astype(BF16), (dp * silu).astype(BF16)


def through_norm(do, wide, scale, da_g, da_u):
    da = (da_g.astype(BF16) + da_u.astype(BF16)).astype(F32)
    by_scale = jnp.sum(da * wide, -1, keepdims=True)
    by_square = (-1.0 / wide.shape[-1]) * by_scale * (scale * scale * scale)
    return do + (da * scale + wide * by_square).astype(BF16)


def put_out(pairs, stage, sem):
    copies = []
    for k, (piece, out) in enumerate(pairs):
        if k >= 2:
            copies[k - 2].wait()
        stage[k % 2] = piece()
        copies.append(pltpu.make_async_copy(stage.at[k % 2], out, sem.at[k % 2]))
        copies[k].start()
    for c in copies[-2:]:
        c.wait()


def flats(total, out, step):
    def piece(k):
        return lambda: total[:, k * step:(k + 1) * step].astype(BF16).T
    return [(piece(k), out.at[pl.ds(k * step, step)]) for k in range(total.shape[1] // step)]


def plains(total, out, step):
    def piece(k):
        return lambda: total[:, k * step:(k + 1) * step].astype(BF16)
    return [(piece(k), out.at[:, pl.ds(k * step, step)]) for k in range(total.shape[1] // step)]


def backward_last(h, dout, wg, wu, wd, tile, step):
    tokens, d = h.shape
    ff = wg.shape[1]
    tiles = tokens // tile

    def kernel(h_ref, do_ref, wg_ref, wu_ref, wd_ref, dh_ref, dwd_out, dwg_out, dwu_out, dwd, dwg, dwu, stage, flat, sem):
        i = pl.program_id(0)

        @pl.when(i == 0)
        def _():
            for total in (dwd, dwg, dwu):
                total[...] = jnp.zeros_like(total)

        do = do_ref[...]
        wide, scale, a = scaled(h_ref[...])
        do_t, a_t = do.T, a.T
        da_g = jnp.zeros((tile, d), F32)
        da_u = jnp.zeros((tile, d), F32)
        for c in range(0, ff, step):
            part = slice(c, c + step)
            p, dg, du = hidden(dot(a, wg_ref[:, part]), dot(a, wu_ref[:, part]), do, wd_ref, part)
            da_g += dot_nt(dg, wg_ref[:, part])
            da_u += dot_nt(du, wu_ref[:, part])
            dwd[:, part] += dot(do_t, p)
            dwg[:, part] += dot(a_t, dg)
            dwu[:, part] += dot(a_t, du)
        dh_ref[...] = through_norm(do, wide, scale, da_g, da_u)

        @pl.when(i == tiles - 1)
        def _():
            put_out(flats(dwd, dwd_out, step), flat, sem)
            put_out(plains(dwg, dwg_out, step) + plains(dwu, dwu_out, step), stage, sem)

    rows = pl.BlockSpec((tile, d), lambda i: (i, 0))
    any_ = pl.BlockSpec(memory_space=ANY)
    return pl.pallas_call(
        kernel, grid=(tiles,), out_shape=[jax.ShapeDtypeStruct(s, BF16) for s in (h.shape, wd.shape, wg.shape, wu.shape)],
        in_specs=[rows, rows, whole(wg.shape), whole(wu.shape), whole(wd.shape)], out_specs=[rows, any_, any_, any_],
        scratch_shapes=[pltpu.VMEM((d, ff), F32)] * 3
        + [pltpu.VMEM((2, d, step), BF16), pltpu.VMEM((2, step, d), BF16), pltpu.SemaphoreType.DMA((2,))],
        name="backward_last",
        cost_estimate=pl.CostEstimate(flops=16 * tokens * d * ff, bytes_accessed=8 * tokens * d + 12 * d * ff, transcendentals=0),
        compiler_params=pltpu.CompilerParams(vmem_limit_bytes=LIMIT))(h, dout, wg, wu, wd)


def reducing(kernel, n, terms, cid, name, grid, args, in_specs, outs, out_specs, scratch, flops):
    A, O, S, M = len(args), len(outs), len(scratch), len(terms)

    def body(*refs):
        at = [0]

        def take(k):
            at[0] += k
            return refs[at[0] - k:at[0]]

        ins, given, results, sums, own = take(A), take(M), take(O), take(M), take(S)
        rest = refs[at[0]:]
        kernel(ins, results, own, Reduce(n, given, sums, rest[:-3], rest[-3:]).stages())

    out = reduced(terms, n)
    return pl.pallas_call(
        body, grid=grid, out_shape=outs + out, in_specs=in_specs + [pl.BlockSpec(memory_space=ANY)] * M,
        out_specs=out_specs + [whole(o.shape) for o in out], scratch_shapes=scratch + Reduce.scratch([t.shape for t in terms], n),
        name=name, cost_estimate=pl.CostEstimate(flops=flops, bytes_accessed=flops // 1000, transcendentals=0),
        compiler_params=pltpu.CompilerParams(collective_id=cid, has_side_effects=True, vmem_limit_bytes=LIMIT))(*args, *terms)


def backward_hidden(n, h, dout, gate, up, wd, terms, tile, step):
    tokens, d = h.shape
    ff = wd.shape[0]
    tiles = tokens // tile
    when = [round(f * (tiles - 1)) for f in (0, 0.47, 0.74, 0.87, 1)]

    def kernel(ins, results, own, stages):
        h_ref, do_ref, gate_ref, up_ref, wd_ref = ins
        dwd_out, at_ref, dg_ref, du_ref = results
        dwd, flat, sem = own
        i = pl.program_id(0)
        spread(stages[:-1], when[:-1])

        @pl.when(i == 0)
        def _():
            dwd[...] = jnp.zeros_like(dwd)

        do = do_ref[...]
        _, _, a = scaled(h_ref[...])
        do_t = do.T
        at_ref[...] = a.T
        for c in range(0, ff, step):
            part = slice(c, c + step)
            p, dg_ref[:, part], du_ref[:, part] = hidden(gate_ref[:, part], up_ref[:, part], do, wd_ref, part)
            dwd[:, part] += dot(do_t, p)

        @pl.when(i == tiles - 1)
        def _():
            put_out(flats(dwd, dwd_out, step), flat, sem)

        spread(stages[-1:], when[-1:])

    rows = pl.BlockSpec((tile, d), lambda i: (i, 0))
    broad = pl.BlockSpec((tile, ff), lambda i: (i, 0))
    shapes = [(ff, d), (d, tokens), (tokens, ff), (tokens, ff)]
    return reducing(
        kernel, n, terms, 3, "backward_hidden", (tiles,), (h, dout, gate, up, wd),
        [rows, rows, broad, broad, whole(wd.shape)], [jax.ShapeDtypeStruct(s, BF16) for s in shapes],
        [pl.BlockSpec(memory_space=ANY), pl.BlockSpec((d, tile), lambda i: (0, i)), broad, broad],
        [pltpu.VMEM((d, ff), F32), pltpu.VMEM((2, step, d), BF16), pltpu.SemaphoreType.DMA((2,))], 4 * tokens * d * ff)


def backward_tail(n, h, dout, a_t, dg, du, wg, wu, older, dwd, tile, step):
    tokens, d = h.shape
    ff = dg.shape[1]
    half, tiles = ff // step, tokens // tile
    full = 2 * half
    late = tiles / 16
    whens = [[round(f * half / 9) for f in (0, 5, 9, 11, 14)],
             [round(f * half / 9) for f in (3, 9, 13, 15, 17)],
             [round(f * half / 9) for f in (9, 16)] + [full + round(f * late) for f in (2, 4, 6)],
             [full + round(f * late) for f in (0, 5, 9, 11, 13)]]
    terms = (older, dwd, *[jax.ShapeDtypeStruct((d, ff), BF16)] * 2)
    out = reduced(terms, n)

    def kernel(h_ref, do_ref, dg_ref, du_ref, wg_ref, wu_ref, at_ref, dgc_ref, duc_ref, older_ref, dwd_ref,
               dx_ref, dwg_ref, dwu_ref, *refs):
        sums, (stage, sem), rest = refs[:4], refs[4:6], refs[6:]
        i = pl.program_id(0)

        def place(ref, k):
            return pltpu.make_async_copy(stage, ref.at[:, pl.ds(pl.multiple_of(k * step, 128), step)], sem)

        @pl.when((i >= 1) & (i <= half))
        def _():
            place(dwg_ref, i - 1).wait()

        @pl.when((i >= half + 1) & (i <= full))
        def _():
            place(dwu_ref, i - 1 - half).wait()

        for k, ref in enumerate((older_ref, dwd_ref, dwg_ref, dwu_ref)):
            spread(Reduce(n, [ref], [sums[k]], rest[11 * k:11 * k + 8], rest[11 * k + 8:11 * k + 11], k == 0).stages(), whens[k])

        @pl.when(i < half)
        def _():
            stage[...] = dot(at_ref[...], dgc_ref[...]).astype(BF16)
            place(dwg_ref, i).start()

        @pl.when((i >= half) & (i < full))
        def _():
            stage[...] = dot(at_ref[...], duc_ref[...]).astype(BF16)
            place(dwu_ref, i - half).start()

        @pl.when(i >= full)
        def _():
            wide, scale, _ = scaled(h_ref[...])
            dx_ref[...] = through_norm(do_ref[...], wide, scale, dot_nt(dg_ref[...], wg_ref[...]), dot_nt(du_ref[...], wu_ref[...]))

    row = lambda i: (jnp.maximum(i - full, 0), 0)
    rows, broad = pl.BlockSpec((tile, d), row), pl.BlockSpec((tile, ff), row)
    any_ = pl.BlockSpec(memory_space=ANY)
    scratch = [pltpu.VMEM((d, step), BF16), pltpu.SemaphoreType.DMA]
    for t in terms:
        scratch += Reduce.scratch([t.shape], n)
    dx, _, _, *sums = pl.pallas_call(
        kernel, grid=(full + tiles,), out_shape=[jax.ShapeDtypeStruct(h.shape, BF16), *terms[2:], *out],
        in_specs=[rows, rows, broad, broad, whole(wg.shape), whole(wu.shape), whole(a_t.shape),
                  pl.BlockSpec((tokens, step), lambda i: (0, jnp.minimum(i, half - 1))),
                  pl.BlockSpec((tokens, step), lambda i: (0, jnp.clip(i - half, 0, half - 1))), any_, any_],
        out_specs=[rows, any_, any_] + [whole(o.shape) for o in out], scratch_shapes=scratch, name="backward_tail",
        cost_estimate=pl.CostEstimate(flops=8 * tokens * d * ff, bytes_accessed=8 * tokens * ff, transcendentals=0),
        compiler_params=pltpu.CompilerParams(collective_id=4, has_side_effects=True, vmem_limit_bytes=LIMIT))(
            h, dout, dg, du, wg, wu, a_t, dg, du, older, dwd)
    return dx, *sums


def solution(mesh):
    n = mesh.shape["dp"]
    if math.isqrt(n) ** 2 != n or math.isqrt(n) != 4:
        raise ValueError("not 4 by 4")

    def step(x, dy, wg, wu, wd):
        shape = x.shape
        x, dy = x[0], dy[0]
        shards = (wg, wu, wd)
        w0 = gather(n, 0, shards)
        h1, gate, up, *w1 = forward(n, x, *w0, shards, 512, 768)
        dh, dwd1, dwg1, dwu1 = backward_last(h1, dy, *w1, 512, 768)
        dwd0, a_t, dg, du, dwd1, dwg1 = backward_hidden(n, x, dh, gate, up, w0[2], [dwd1, dwg1], 256, 768)
        dx, dwu1, dwd0, dwg0, dwu0 = backward_tail(n, x, dh, a_t, dg, du, *w0[:2], dwu1, dwd0, 256, 256)
        return (dx.reshape(shape), jnp.stack((dwg0, dwg1)), jnp.stack((dwu0, dwu1)), jnp.stack((dwd0, dwd1)))

    tokens = P(("rep", "dp"), None, None)
    rows = P(None, "dp", None)
    by = P("rep", "dp", None)
    return jax.shard_map(step, mesh=mesh, in_specs=(tokens, tokens, rows, rows, rows), out_specs=(tokens, by, by, by), check_vma=False)
```
